32 devices in a mesh: ep: 4 (over y, x), tp: 8 (over z, core).
Axes of the slice: x: 2, y: 2, z: 4, core: 2. Of those that a mesh axis runs over, the one named last changes fastest.
Arguments:
- tokens: bfloat16 [512, 6144], P('ep'), may hold values from -6 to 6
- expert_ids: int32 [512, 2], P('ep'), may hold values from 0 to 3, all different within a row; in each aligned block of 128 rows (0 to 127, 128 to 255, ...) at most 96 rows name the same one
- router: bfloat16 [6144, 4], replicated, may hold values from -0.078125 to 0.078125
- gate_weight: bfloat16 [4, 6144, 8192], P('ep', None, 'tp'), may hold values from -0.078125 to 0.078125
- up_weight: bfloat16 [4, 6144, 8192], P('ep', None, 'tp'), may hold values from -0.078125 to 0.078125
- down_weight: bfloat16 [4, 8192, 6144], P('ep', 'tp'), may hold values from -0.0625 to 0.0625
- keep_mask: int32 [512, 6144], P('ep'), may hold values 0 or 1
Outputs:
- layer_out: bfloat16 [512, 6144], P('ep')
The draws below stay inside these ranges and needn't reach their ends.
Inputs may be any that keep to these rules, and one draw needn't show every extreme that they name: `expert_ids`: each row names two different experts. In the rows of one token block of 128 rows no expert is named more than 96 times, a bound that some block reaches.
All inputs are finite; a program needn't handle non-finite values. No bound on the sum of `keep_mask` on one device may be relied on, other than what follows from the above.
Results may differ from the reference program's by a relative error of at most 0.018.
Values may be sent and summed in bfloat16 or wider, within the bound.
A program may use at most 128 MiB of HBM per device.

```python
import math
import jax
import jax.numpy as jnp
import numpy as np
from jax import lax

D = 6144
FF = 8192
TOK_DEV = 128
EXPERTS = 4
CAP = 96
TOKENS = 512
N_EP = 4
N_TP = 8


def set_ends(drawn, rng, smallest, top_value):
    index_at = [jax.random.randint(jax.random.fold_in(rng, axis), (), 0, length) for axis, length in enumerate(drawn.shape)]
    longest = drawn.shape.index(max(drawn.shape))
    next_to = index_at[:longest] + [(index_at[longest] + 1) % drawn.shape[longest]] + index_at[longest + 1:]
    return drawn.at[tuple(index_at)].set(smallest).at[tuple(next_to)].set(top_value)


def levels(key, extent, pieces, least, largest):
    def one(dim, shards_of):
        steps = jax.random.uniform(jax.random.fold_in(jax.random.fold_in(key, 6), dim), (shards_of,), jnp.float32, least / len(pieces), largest / len(pieces))
        return jnp.repeat(jnp.exp(steps), extent[dim] // shards_of).reshape((-1,) + (1,) * (len(extent) - dim - 1))

    gain = one(*pieces[0])
    for cut in pieces[1:]:
        gain = gain * one(*cut)
    return gain


def assign_block(key, own, number, rows, count, top, limit, skew):
    ranking = jax.random.permutation(key, count)
    heavy_load, ordinary = shares(count, rows * top, limit, skew, True), shares(count, rows * top, limit, skew, False)
    places = jnp.arange(count)

    def named(tallies, offset_by):
        used = int((tallies > 0).sum())
        fixed = max(1, used // 4)
        moved = fixed + (places - fixed + offset_by * (used - fixed)) % max(1, count - fixed)
        return jnp.zeros((count,), jnp.int32).at[ranking[jnp.where(places < fixed, places, moved)]].set(jnp.asarray(tallies, jnp.int32))

    tallies = jnp.where(number % 4 == 0, named(heavy_load, number // 4), named(ordinary, number - number // 4 - 1))
    mixed = jax.random.permutation(jax.random.fold_in(own, 3), count)
    source_of, receiver = mixed[0:count // 2 * 2:2], mixed[1:count // 2 * 2:2]
    slack = jnp.minimum(tallies[source_of] - 1, limit - tallies[receiver]) // 2
    slack = jnp.where((source_of == ranking[0]) | (receiver == ranking[0]) | (tallies[receiver] == 0), 0, jnp.maximum(slack, 0))
    moved = jax.random.randint(jax.random.fold_in(own, 4), (count // 2,), 0, 1 << 20) % (slack + 1)
    tallies = tallies.at[source_of].add(-moved).at[receiver].add(moved)
    labels = jnp.searchsorted(jnp.cumsum(tallies), jnp.arange(rows * top), side="right").astype(jnp.int32)
    listing = labels.reshape(top, rows).T
    listing = listing[jax.random.permutation(jax.random.fold_in(own, 1), rows)]
    offset_by = jax.random.randint(jax.random.fold_in(own, 2), (rows, 1), 0, top)
    return jnp.take_along_axis(listing, (jnp.arange(top)[None, :] + offset_by) % top, axis=1)


def shares(count, total, bound, slope, full):
    weights = [(1 << 20) // math.isqrt(rank ** slope) + 1 for rank in range(1, count + 1)]
    largest = bound if full else min(bound, max(-(-total // count), total * weights[0] // sum(weights)))
    least = 1 if total - largest >= count - 1 else 0
    holding, rest = [largest] + [least] * (count - 1), total - largest - least * (count - 1)
    while rest > 0:
        movable = [i for i in range(1, count) if holding[i] < largest] or [i for i in range(1, count) if holding[i] < bound]
        mass, budget = sum([weights[i] for i in movable]), rest
        for i in movable:
            more = min(bound - holding[i], max(1, budget * weights[i] // mass), rest)
            holding[i] = holding[i] + more
            rest = rest - more
    return np.array(holding)


def centred(own_key, extent, spread, limit, split=(), kind=jnp.bfloat16):
    values = jax.random.normal(own_key, extent, jnp.float32) * spread
    if len(split) > 0:
        values = levels(own_key, extent, split, -0.22, 0.18) * values
    return jnp.clip(values, min=-limit, max=limit).astype(kind)


def setup_inputs(seed: int = 0) -> dict:
    splits = jax.random.split(jax.random.key(seed), 8)
    tokens = centred(splits[0], (TOKENS, D), 1.0, 6.0, ((0, 4),))
    expert_ids_keys = jax.random.split(jax.random.fold_in(splits[1], 1), TOKENS // TOK_DEV)
    expert_ids_turns = jax.random.permutation(jax.random.fold_in(splits[1], 3), TOKENS // TOK_DEV)
    expert_ids = jax.vmap(lambda own, number: assign_block(jax.random.fold_in(splits[1], 2), own, number, TOK_DEV, EXPERTS, 2, CAP, 2))(expert_ids_keys, expert_ids_turns).reshape((TOKENS, 2))
    router = centred(splits[2], (D, EXPERTS), D ** -0.5, 0.078125)
    gate_weight = centred(splits[3], (EXPERTS, D, FF), D ** -0.5, 0.078125, ((0, 4), (2, 8)))
    up_weight = centred(splits[4], (EXPERTS, D, FF), D ** -0.5, 0.078125, ((0, 4), (2, 8)))
    down_weight = centred(splits[5], (EXPERTS, FF, D), FF ** -0.5, 0.0625, ((0, 4), (1, 8)))
    keep_mask = set_ends((jax.random.randint(splits[6], (TOKENS, D), 0, 5) < 4).astype(jnp.int32), jax.random.fold_in(splits[6], 1), 0, 1)
    return dict(tokens=tokens, expert_ids=expert_ids, router=router, gate_weight=gate_weight, up_weight=up_weight, down_weight=down_weight, keep_mask=keep_mask)


def reference(tokens, expert_ids, router, gate_weight, up_weight, down_weight, keep_mask):
    total_rows = tokens.shape[0]
    logits = jnp.dot(tokens, router, preferred_element_type=jnp.float32)
    picked = jnp.take_along_axis(logits, expert_ids, axis=1)
    weight_first = jax.nn.sigmoid(picked[:, 0] - picked[:, 1])
    weight_second = jax.nn.sigmoid(picked[:, 1] - picked[:, 0])
    onehot = (expert_ids[:, :, None] == jnp.arange(EXPERTS, dtype=jnp.int32)[None, None, :]).astype(jnp.int32)
    blocked = onehot.reshape(N_EP, TOK_DEV * 2, EXPERTS)
    ranks = jnp.cumsum(blocked, axis=1) - blocked
    slot = jnp.sum(ranks * blocked, axis=2).reshape(total_rows, 2)
    block_of = jnp.arange(total_rows, dtype=jnp.int32) // TOK_DEV
    place = (block_of[:, None] * CAP + slot).astype(jnp.int32)
    token_index = jnp.broadcast_to(jnp.arange(total_rows, dtype=jnp.int32)[:, None], (total_rows, 2))
    table = jnp.full((EXPERTS, N_EP * CAP), total_rows, jnp.int32)
    table = table.at[expert_ids, place].set(token_index)
    padded = jnp.concatenate([tokens, jnp.zeros((1, tokens.shape[1]), jnp.bfloat16)], axis=0)
    width = FF // N_TP

    def one_expert(inputs):
        w_gate, w_up, w_down, rows_index = inputs
        buffer = jnp.take(padded, rows_index, axis=0)
        gate = jnp.dot(buffer, w_gate, preferred_element_type=jnp.float32)
        up = jnp.dot(buffer, w_up, preferred_element_type=jnp.float32)
        hidden = (jax.nn.silu(gate) * up).astype(jnp.bfloat16)

        def add_block(block, total):
            start = (block * width).astype(jnp.int32)
            h_block = lax.dynamic_slice_in_dim(hidden, start, width, 1)
            d_block = lax.dynamic_slice_in_dim(w_down, start, width, 0)
            partial_sum = jnp.dot(h_block, d_block, preferred_element_type=jnp.float32)
            rounded = lax.optimization_barrier(partial_sum.astype(jnp.bfloat16))
            return total + rounded.astype(jnp.float32)

        empty = jnp.zeros((buffer.shape[0], buffer.shape[1]), jnp.float32)
        summed = lax.fori_loop(0, N_TP, add_block, empty)
        return summed.astype(jnp.bfloat16)

    outputs = lax.map(one_expert, (gate_weight, up_weight, down_weight, table))
    first_rows = outputs[expert_ids[:, 0], place[:, 0]].astype(jnp.float32)
    second_rows = outputs[expert_ids[:, 1], place[:, 1]].astype(jnp.float32)
    combined = weight_first[:, None] * first_rows + weight_second[:, None] * second_rows
    return (combined * keep_mask.astype(jnp.float32) * 1.25).astype(jnp.bfloat16)
```

```python
import functools

import jax
import jax.numpy as jnp
from jax import lax
from jax.experimental import pallas as pl
from jax.experimental.pallas import tpu as pltpu
from jax.sharding import PartitionSpec as P

MESH = pl.DeviceIdType.MESH


def flip(index, offset, count):
    out, bit = 0, 1
    while bit < count:
        out = out + ((index // bit + offset // bit) % 2) * bit
        bit *= 2
    return out


def kernel(
    n_ep, nz, slots_ref, comb_ref, gate_hbm, up_hbm, down_hbm, mask_hbm, out_ref,
    w_gate, w_up, w_down, mask, rows, hidden, pair_out, pair_in, mine, ep_out, ep_in,
    z_out, z_in, acc, local_sem, mask_sem, disp_s, disp_r, fwd_s, fwd_r, pair_s, pair_r, ep_s, ep_r,
    z_s, z_r, b_s, b_r, gfw_s, gfw_r,
):
    ep, tp = lax.axis_index("ep"), lax.axis_index("tp")
    z, core = tp // 2, tp % 2
    partner = (ep, z * 2 + (1 - core))
    cap, width = rows.shape[1], rows.shape[2]
    toks = out_ref.shape[0]
    ff = w_gate.shape[1]
    half = width // 2
    steps, sub = pair_in.shape[0], pair_in.shape[2]

    def cols(owner_core, s):
        return pl.ds(pl.multiple_of(owner_core * half + s * sub, 128), sub)

    def root_of(s):
        return max(0, nz // 2 - 1) + (s % 2 if nz > 1 else 0)

    load_own = pltpu.make_async_copy(slots_ref.at[ep], rows.at[0], local_sem.at[0])
    load_gate = pltpu.make_async_copy(gate_hbm, w_gate, local_sem.at[1])
    load_up = pltpu.make_async_copy(up_hbm, w_up, local_sem.at[2])
    load_down = pltpu.make_async_copy(down_hbm, w_down, local_sem.at[3])
    odd_root = jnp.clip(z - root_of(0), 0, 1)
    load_mask = [pltpu.make_async_copy(mask_hbm.at[:, cols(core, 2 * j + odd_root)], mask.at[j], mask_sem.at[j])
                 for j in range(mask.shape[0])]
    for load in (load_own, load_gate, load_up):
        load.start()

    barrier = pltpu.get_barrier_semaphore()
    peers = [(flip(ep, o, n_ep), tp) for o in range(1, n_ep)]
    peers += [(ep, ((z + s) % nz) * 2 + core) for s in range(1, nz)] + [partner]
    for peer in peers:
        pl.semaphore_signal(barrier, inc=1, device_id=peer, device_id_type=MESH)
    pl.semaphore_wait(barrier, len(peers))

    def remote(src, dst, send, recv, device):
        return pltpu.make_async_remote_copy(
            src_ref=src, dst_ref=dst, send_sem=send, recv_sem=recv,
            device_id=device, device_id_type=MESH,
        )

    started = []

    third = half // 3
    odd = z % 2
    z_pair = (ep, (z + 1 - 2 * odd) * 2 + core)

    def part(which):
        return pl.ds(pl.multiple_of(core * half + which * third, 128), third)

    shared, common, foreign = part(2 * odd), part(1), part(2 - 2 * odd)
    arrive, forward = {}, {}

    def send_rows(o, kind, at):
        peer = flip(ep, o, n_ep)
        copy = remote(slots_ref.at[peer, :, at], rows.at[o, :, at],
                      disp_s.at[kind, o], disp_r.at[kind, o], (peer, tp))
        copy.start()
        arrive[kind, o] = copy
        started.append(copy)

    def pass_on(o, kind, at):
        arrive[kind, o].wait_recv()
        if kind == 0:
            copy = remote(rows.at[o, :, at], rows.at[o, :, at],
                          disp_s.at[2, o], disp_r.at[2, o], z_pair)
            copy.start()
            arrive[2, o] = copy
            started.append(copy)
        copy = remote(rows.at[o, :, at], rows.at[o, :, at],
                      fwd_s.at[kind, o], fwd_r.at[kind, o], partner)
        copy.start()
        forward[kind, o] = copy
        started.append(copy)

    share_order = [n_ep - 1] + list(range(1, n_ep - 1))
    for o in share_order:
        send_rows(o, 0, shared)
    for o in range(1, n_ep):
        send_rows(o, 1, common)
    load_down.start()
    for load in load_mask:
        load.start()
    for o in share_order:
        pass_on(o, 0, shared)

    tile = min(256, ff)
    phases = 2
    per = n_ep // phases
    for phase in range(phases):
        for o in range(phase * per, (phase + 1) * per):
            if o > 0:
                pass_on(o, 1, common)
                pass_on(o, 2, foreign)
        if phase == 0:
            load_own.wait()
            load_gate.wait()
            load_up.wait()
        for o in range(phase * per, (phase + 1) * per):
            if o > 0:
                for kind in range(3):
                    forward[kind, o].wait_recv()

        def up_step(t, carry):
            at = pl.ds(pl.multiple_of(t * tile, tile), tile)
            block = rows[phase * per:(phase + 1) * per].reshape(per * cap, width)
            gate = jnp.dot(block, w_gate[:, at], preferred_element_type=jnp.float32)
            up = jnp.dot(block, w_up[:, at], preferred_element_type=jnp.float32)
            hidden[phase * per * cap:(phase + 1) * per * cap, at] = (
                jax.nn.silu(gate) * up).astype(jnp.bfloat16)
            return carry

        lax.fori_loop(0, ff // tile, up_step, 0)

    load_down.wait()
    for load in load_mask:
        load.wait()

    ep_lag, z_lag = 3, 2
    depth = max(root_of(0), nz - 1 - root_of(0), root_of(1), nz - 1 - root_of(1))
    pair, exchange = [], [[] for _ in range(steps)]

    def pair_sum(s):
        pair[s].wait_recv()
        summed = (mine[s % 2].astype(jnp.float32) + pair_in[s].astype(jnp.float32)).astype(jnp.bfloat16)
        ep_in[s, 0:cap, :] = summed[0:cap]
        ep_out[s] = summed[cap:]
        for o in range(1, n_ep):
            copy = remote(ep_out.at[s, pl.ds((o - 1) * cap, cap), :], ep_in.at[s, pl.ds(o * cap, cap), :],
                          ep_s.at[s, o], ep_r.at[s, o], (flip(ep, o, n_ep), tp))
            copy.start()
            exchange[s].append(copy)
            started.append(copy)

    def inward(s, root):
        side = jnp.where(z < root, 0, 1)
        to = jnp.where(z < root, z + 1, z - 1)
        return remote(z_out.at[s], z_in.at[s, side], z_s.at[s], z_r.at[s, side], (ep, to * 2 + core))

    def from_side(s, side):
        return remote(z_out.at[s], z_in.at[s, side], z_s.at[s], z_r.at[s, side], partner)

    def outward(s, side):
        here = out_ref.at[:, cols(core, s)]
        return remote(here, here, b_s.at[s, side], b_r.at[s], (ep, (z - 1 + 2 * side) * 2 + core))

    def to_partner(s):
        here = out_ref.at[:, cols(core, s)]
        return remote(here, here, gfw_s.at[s], gfw_r.at[s], partner)

    def combine(s):
        for copy in exchange[s]:
            copy.wait_recv()
        both = jnp.dot(comb_ref[...], ep_in[s], preferred_element_type=jnp.float32)
        acc[s % acc.shape[0]] = both[0:toks] + both[toks:]

    def chain(s, k):
        root = root_of(s)
        top = max(root, nz - 1 - root)
        held = s % acc.shape[0]
        if k < top:

            @pl.when(((z < root) & (z == k)) | ((z > root) & (nz - 1 - z == k)))
            def _():
                total = acc[held]
                if k > 0:
                    side = jnp.where(z < root, 0, 1)
                    from_side(s, side).wait_recv()
                    total = total + z_in[s, side].astype(jnp.float32)
                z_out[s] = total.astype(jnp.bfloat16)
                inward(s, root).start()

        elif k == top:

            @pl.when(z == root)
            def _():
                total = acc[held]
                for side in range(2):
                    if (root > 0, root < nz - 1)[side]:
                        from_side(s, side).wait_recv()
                        total = total + z_in[s, side].astype(jnp.float32)
                keep = mask[s // 2].astype(jnp.float32)
                out_ref[:, cols(core, s)] = (total * keep * 1.25).astype(jnp.bfloat16)
                if root > 0:
                    outward(s, 0).start()
                if root < nz - 1:
                    outward(s, 1).start()
                to_partner(s).start()

        else:
            away = k - top

            @pl.when((z == root - away) | (z == root + away))
            def _():
                outward(s, 0).wait_recv()

                @pl.when((z < root) & (z > 0))
                def _():
                    outward(s, 0).start()

                @pl.when((z > root) & (z < nz - 1))
                def _():
                    outward(s, 1).start()

                to_partner(s).start()

    def advance(i):
        for k in range(2 * depth, 0, -1):
            s = i - ep_lag - k * z_lag
            if 0 <= s < steps and k <= 2 * max(root_of(s), nz - 1 - root_of(s)):
                chain(s, k)
        s = i - ep_lag
        if 0 <= s < steps:
            combine(s)
            chain(s, 0)

    for s in range(steps):
        pair_out[s] = jnp.dot(hidden[...], w_down[:, cols(1 - core, s)],
                              preferred_element_type=jnp.float32).astype(jnp.bfloat16)
        copy = remote(pair_out.at[s], pair_in.at[s], pair_s.at[s], pair_r.at[s], partner)
        copy.start()
        pair.append(copy)
        started.append(copy)
        if s > 0:
            pair_sum(s - 1)
        mine[s % 2] = jnp.dot(hidden[...], w_down[:, cols(core, s)],
                              preferred_element_type=jnp.float32).astype(jnp.bfloat16)
        advance(s)
    pair_sum(steps - 1)

    for i in range(steps, steps + ep_lag + 2 * depth * z_lag + 1):
        advance(i)
    for s in range(steps):
        to_partner(s).wait_recv()
    for copy in started:
        copy.wait_send()
    for s in range(steps):
        root = root_of(s)

        @pl.when(z != root)
        def _():
            inward(s, root).wait_send()

        @pl.when((z <= root) & (z > 0))
        def _():
            outward(s, 0).wait_send()

        @pl.when((z >= root) & (z < nz - 1))
        def _():
            outward(s, 1).wait_send()

        to_partner(s).wait_send()


def shards(n_ep, n_tp, tokens, expert_ids, router, gate_weight, up_weight, down_weight, keep_mask):
    experts = router.shape[1]
    toks, width = tokens.shape
    cap = 3 * toks // experts
    nz = n_tp // 2
    total = experts * cap
    sub = 256
    steps = width // 2 // sub
    logits = jnp.dot(tokens, router, preferred_element_type=jnp.float32)
    numbers = jnp.arange(experts, dtype=jnp.int32)
    onehot3 = expert_ids[:, :, None] == numbers[None, None, :]
    picked = jnp.sum(jnp.where(onehot3, logits[:, None, :], 0.0), axis=2)
    weight_first = jax.nn.sigmoid(picked[:, 0] - picked[:, 1])
    weight_second = jax.nn.sigmoid(picked[:, 1] - picked[:, 0])
    onehot = onehot3.astype(jnp.float32)
    named = onehot[:, 0] + onehot[:, 1]
    order = jnp.arange(toks, dtype=jnp.int32)
    before = (order[None, :] < order[:, None]).astype(jnp.bfloat16)
    ranks = jnp.dot(before, named.astype(jnp.bfloat16), preferred_element_type=jnp.float32)
    slot = jnp.sum(ranks[:, None, :] * onehot, axis=2).astype(jnp.int32)
    lines = jnp.arange(total, dtype=jnp.int32)
    place = expert_ids * cap + slot
    picker = ((place[None, :, 0] == lines[:, None]) | (place[None, :, 1] == lines[:, None])).astype(jnp.bfloat16)
    slots = jnp.dot(picker, tokens, preferred_element_type=jnp.float32).astype(jnp.bfloat16)
    slots = slots.reshape(experts, cap, width)
    turned = jnp.bitwise_xor(expert_ids, lax.axis_index("ep")) * cap + slot
    comb = (jnp.where(turned[:, 0:1] == lines[None, :], weight_first[:, None], 0.0)
            + jnp.where(turned[:, 1:2] == lines[None, :], weight_second[:, None], 0.0))
    high = lax.reduce_precision(comb, 8, 7)
    comb = jnp.concatenate([high, comb - high], axis=0).astype(jnp.bfloat16)
    w_gate, w_up, w_down = gate_weight[0], up_weight[0], down_weight[0]
    ff = w_gate.shape[1]
    vmem, hbm = pl.BlockSpec(memory_space=pltpu.VMEM), pl.BlockSpec(memory_space=pl.ANY)
    bf = jnp.bfloat16
    dma = pltpu.SemaphoreType.DMA
    return pl.pallas_call(
        functools.partial(kernel, n_ep, nz),
        out_shape=jax.ShapeDtypeStruct((toks, width), bf),
        in_specs=[vmem, vmem, hbm, hbm, hbm, hbm],
        out_specs=vmem,
        scratch_shapes=[
            pltpu.VMEM((width, ff), bf), pltpu.VMEM((width, ff), bf), pltpu.VMEM((ff, width), bf),
            pltpu.VMEM((steps // 2, toks, sub), jnp.int32),
            pltpu.VMEM((experts, cap, width), bf),
            pltpu.VMEM((total, ff), bf),
            pltpu.VMEM((steps, total, sub), bf), pltpu.VMEM((steps, total, sub), bf),
            pltpu.VMEM((2, total, sub), bf),
            pltpu.VMEM((steps, total - cap, sub), bf), pltpu.VMEM((steps, total, sub), bf),
            pltpu.VMEM((steps, toks, sub), bf), pltpu.VMEM((steps, 2, toks, sub), bf),
            pltpu.VMEM((8, toks, sub), jnp.float32),
            dma((4,)), dma((steps // 2,)),
            dma((3, n_ep)), dma((3, n_ep)), dma((3, n_ep)), dma((3, n_ep)),
            dma((steps,)), dma((steps,)), dma((steps, n_ep)), dma((steps, n_ep)),
            dma((steps,)), dma((steps, 2)), dma((steps, 2)), dma((steps,)),
            dma((steps,)), dma((steps,)),
        ],
        compiler_params=pltpu.CompilerParams(
            collective_id=0, has_side_effects=True, vmem_limit_bytes=67043328),
    )(slots, comb, w_gate, w_up, w_down, keep_mask)


def solution(mesh):
    return jax.shard_map(
        functools.partial(shards, mesh.shape["ep"], mesh.shape["tp"]),
        mesh=mesh,
        in_specs=(
            P("ep", None),
            P("ep", None),
            P(),
            P("ep", None, "tp"),
            P("ep", None, "tp"),
            P("ep", "tp", None),
            P("ep", None),
        ),
        out_specs=P("ep", None),
        check_vma=False,
    )
```

```python
import functools

import jax
import jax.numpy as jnp
from jax import lax
from jax.experimental import pallas as pl
from jax.experimental.pallas import tpu as pltpu
from jax.sharding import PartitionSpec as P

MESH = pl.DeviceIdType.MESH


def flip(index, offset, count):
    out, bit = 0, 1
    while bit < count:
        out = out + ((index // bit + offset // bit) % 2) * bit
        bit *= 2
    return out


def kernel(
    n_ep, nz, ids_ref, router_ref, tokens_hbm, gate_hbm, up_hbm, down_hbm, mask_hbm, out_ref,
    tokens, w_gate, w_up, w_down, mask, rows, gate_up, hidden, comb, pair_out, pair_in, mine, ep_out, ep_in,
    z_out, z_in, acc, local_sem, w_sem, disp_s, disp_r, share_s, share_r, fwd_s, fwd_r,
    pair_s, pair_r, ep_s, ep_r, z_s, z_r, b_s, b_r, gfw_s, gfw_r,
):
    ep, tp = lax.axis_index("ep"), lax.axis_index("tp")
    z, core = tp // 2, tp % 2
    partner = (ep, z * 2 + (1 - core))
    cap, width = rows.shape[1], rows.shape[2]
    toks = out_ref.shape[0]
    ff = w_gate.shape[1]
    half = width // 2
    steps, sub = pair_in.shape[0], pair_in.shape[2]
    groups = fwd_r.shape[0]
    experts = router_ref.shape[0]
    wide = half // groups
    total_rows = n_ep * cap

    def cols(owner_core, s):
        return pl.ds(pl.multiple_of(owner_core * half + s * sub, 128), sub)

    def root_of(s):
        return max(0, nz // 2 - 1) + (s % 2 if nz > 1 else 0)

    load_tokens = pltpu.make_async_copy(tokens_hbm, tokens, local_sem.at[0])
    load_tokens.start()

    def load_weights(g):
        for h in range(2):
            at = pl.ds(h * half + g * wide, wide)
            for src, dst in ((gate_hbm, w_gate), (up_hbm, w_up)):
                pltpu.make_async_copy(src.at[at], dst.at[at], w_sem.at[g]).start()

    def wait_weights(g):
        at = pl.ds(0, 4 * wide)
        pltpu.make_async_copy(gate_hbm.at[at], w_gate.at[at], w_sem.at[g]).wait()

    load_down = pltpu.make_async_copy(down_hbm, w_down, local_sem.at[1])
    odd_root = jnp.clip(z - root_of(0), 0, 1)
    load_mask = [pltpu.make_async_copy(mask_hbm.at[:, cols(core, 2 * j + odd_root)],
                                       mask.at[:, j * sub:(j + 1) * sub], local_sem.at[2])
                 for j in range(steps // 2)]

    barrier = pltpu.get_barrier_semaphore()
    for peer in [(flip(ep, o, n_ep), tp) for o in range(1, n_ep)] + [partner]:
        pl.semaphore_signal(barrier, inc=1, device_id=peer, device_id_type=MESH)

    @pl.when(z > 0)
    def _():
        pl.semaphore_signal(barrier, inc=1, device_id=(ep, (z - 1) * 2 + core), device_id_type=MESH)

    @pl.when(z < nz - 1)
    def _():
        pl.semaphore_signal(barrier, inc=1, device_id=(ep, (z + 1) * 2 + core), device_id_type=MESH)

    def remote(src, dst, send, recv, device):
        return pltpu.make_async_remote_copy(
            src_ref=src, dst_ref=dst, send_sem=send, recv_sem=recv,
            device_id=device, device_id_type=MESH,
        )

    odd = z % 2
    z_pair = (ep, (z + 1 - 2 * odd) * 2 + core)

    first_id, second_id = ids_ref[0:1, :], ids_ref[1:2, :]
    numbers = lax.broadcasted_iota(jnp.int32, (experts, toks), 0)
    is_first, is_second = numbers == first_id, numbers == second_id
    named = jnp.where(is_first, 1.0, 0.0) + jnp.where(is_second, 1.0, 0.0)
    before = (lax.broadcasted_iota(jnp.int32, (toks, toks), 0) < lax.broadcasted_iota(jnp.int32, (toks, toks), 1))
    ranks = jnp.dot(named.astype(jnp.bfloat16), jnp.where(before, 1.0, 0.0).astype(jnp.bfloat16),
                    preferred_element_type=jnp.float32)

    def of_choice(chosen, values):
        return jnp.sum(jnp.where(chosen, values, 0.0), axis=0, keepdims=True)

    slots = of_choice(is_first, ranks), of_choice(is_second, ranks)
    places = [(number * cap).astype(jnp.float32) + slot for number, slot in zip((first_id, second_id), slots)]

    def picker(owner):
        lines = (lax.broadcasted_iota(jnp.int32, (cap, toks), 0) + owner * cap).astype(jnp.float32)
        return jnp.where((places[0] == lines) | (places[1] == lines), 1.0, 0.0).astype(jnp.bfloat16)

    def piece_of(kind, g):
        return 3 * g + (2 * odd, 1, 2 - 2 * odd)[kind]

    def dispatch(kind, g, o):
        s = piece_of(kind, g)
        return remote(ep_out.at[s, pl.ds((o - 1) * cap, cap), :], rows.at[o, :, cols(core, s)],
                      disp_s.at[0], disp_r.at[kind, g], (flip(ep, o, n_ep), tp))

    def guests(kind, g):
        return rows.at[pl.ds(1, n_ep - 1), :, cols(core, piece_of(kind, g))]

    def share(g):
        return remote(guests(0, g), guests(0, g), share_s.at[0], share_r.at[g], z_pair)

    def forward(kind, g):
        return remote(guests(kind, g), guests(kind, g), fwd_s.at[0], fwd_r.at[g], partner)

    def pass_on(kind, g):
        if kind < 2:
            remote(guests(kind, g), guests(kind, g), disp_s.at[0], disp_r.at[kind, g], partner).wait_recv()
        else:
            share(g).wait_recv()
        if kind == 0:
            share(g).start()
        forward(kind, g).start()

    order = [(0, 0)]
    for g in range(groups):
        if g + 1 < groups:
            order.append((0, g + 1))
        order.append((1, g))
    with jax.named_scope("tokens"):
        load_tokens.wait()
    for g in range(groups):
        load_weights(g)
    others = jnp.concatenate([picker(flip(ep, o, n_ep)) for o in range(1, n_ep)], axis=0)
    for n, (kind, g) in enumerate(order):
        s = piece_of(kind, g)
        ep_out[s] = jnp.dot(others, tokens[:, cols(core, s)],
                            preferred_element_type=jnp.float32).astype(jnp.bfloat16)
        if n == 0:
            peers = n_ep + jnp.where(z > 0, 1, 0) + jnp.where(z < nz - 1, 1, 0)
            with jax.named_scope("barrier"):
                pl.semaphore_wait(barrier, peers)
        for o in [n_ep - 1] + list(range(1, n_ep - 1)):
            dispatch(kind, g, o).start()
    load_down.start()
    for load in load_mask:
        load.start()

    own = picker(ep)
    strip = width // 6
    for n in range(6):
        rows[0, :, n * strip:(n + 1) * strip] = jnp.dot(
            own, tokens[:, n * strip:(n + 1) * strip], preferred_element_type=jnp.float32).astype(jnp.bfloat16)

    logits = lax.dot_general(router_ref[...], tokens[...], (((1,), (1,)), ((), ())),
                             preferred_element_type=jnp.float32)
    ahead = of_choice(is_first, logits) - of_choice(is_second, logits)
    lines = lax.broadcasted_iota(jnp.int32, (total_rows, toks), 0).astype(jnp.float32)
    turned = [(jnp.bitwise_xor(number, ep) * cap).astype(jnp.float32) + slot
              for number, slot in zip((first_id, second_id), slots)]
    mixed = (jnp.where(turned[0] == lines, jax.nn.sigmoid(ahead), 0.0)
             + jnp.where(turned[1] == lines, jax.nn.sigmoid(-ahead), 0.0))
    comb[...] = mixed.T.astype(jnp.bfloat16)

    tile = min(256, ff)
    tiles = ff // tile

    def up_tile(g, n):
        at = slice(n * tile, (n + 1) * tile)
        sums = []
        for i, w in enumerate((w_gate, w_up)):
            part = None
            for h in range(2):
                k = slice(h * half + g * wide, h * half + (g + 1) * wide)
                dot = jnp.dot(rows[:, :, k].reshape(total_rows, wide), w[k, at],
                              preferred_element_type=jnp.float32)
                part = dot if part is None else part + dot
            if g > 0:
                part = part + gate_up[i, :, at]
            if g < groups - 1:
                gate_up[i, :, at] = part
            sums.append(part)
        if g == groups - 1:
            hidden[:, at] = (jax.nn.silu(sums[0]) * sums[1]).astype(jnp.bfloat16)

    todo = []
    for g in range(groups):
        todo += [(0, g), (1, g - 1), (2, g - 1)] if g else [(0, 0)]
    todo += [(1, groups - 1), (2, groups - 1)]
    for g in range(groups):
        with jax.named_scope(f"pass_{g}"):
            while any((kind, g) in todo for kind in range(3)):
                pass_on(*todo.pop(0))
        with jax.named_scope(f"arrive_{g}"):
            wait_weights(g)
            here = rows.at[pl.ds(1, n_ep - 1), :, pl.ds(0, wide)]
            remote(here, here, fwd_s.at[0], fwd_r.at[g], partner).wait_recv()
        with jax.named_scope(f"up_{g}"):
            for n in range(tiles):
                up_tile(g, n)
                if n == tiles // 2 - 1 and todo:
                    pass_on(*todo.pop(0))

    load_down.wait()
    pltpu.make_async_copy(mask_hbm.at[:, 0:mask.shape[1]], mask, local_sem.at[2]).wait()
    staged = ep_out.at[pl.ds(0, len(order))]
    remote(staged, staged, disp_s.at[0], disp_r.at[0, 0], partner).wait_send()

    ep_lag, z_lag = 3, 2
    depth = max(root_of(0), nz - 1 - root_of(0), root_of(1), nz - 1 - root_of(1))
    pair = []

    def pair_sum(s):
        pair[s].wait_recv()
        summed = (mine[s % 2].astype(jnp.float32) + pair_in[s].astype(jnp.float32)).astype(jnp.bfloat16)
        ep_in[s, 0:cap, :] = summed[0:cap]
        ep_out[s] = summed[cap:]
        for o in range(1, n_ep):
            copy = remote(ep_out.at[s, pl.ds((o - 1) * cap, cap), :], ep_in.at[s, pl.ds(o * cap, cap), :],
                          ep_s.at[0], ep_r.at[s], (flip(ep, o, n_ep), tp))
            copy.start()

    def inward(s, root):
        side = jnp.where(z < root, 0, 1)
        to = jnp.where(z < root, z + 1, z - 1)
        return remote(z_out.at[s], z_in.at[s, side], z_s.at[s % 2], z_r.at[s, side], (ep, to * 2 + core))

    def from_side(s, side):
        return remote(z_out.at[s], z_in.at[s, side], z_s.at[s % 2], z_r.at[s, side], partner)

    def outward(s, side):
        here = out_ref.at[:, cols(core, s)]
        return remote(here, here, b_s.at[s % 2, side], b_r.at[s], (ep, (z - 1 + 2 * side) * 2 + core))

    def to_partner(s):
        here = out_ref.at[:, cols(core, s)]
        return remote(here, here, gfw_s.at[0], gfw_r.at[0], partner)

    def combine(s):
        arrived = ep_in.at[s, pl.ds(cap, total_rows - cap), :]
        remote(arrived, arrived, ep_s.at[0], ep_r.at[s], partner).wait_recv()
        acc[s % acc.shape[0]] = jnp.dot(comb[...], ep_in[s], preferred_element_type=jnp.float32)

    def chain(s, k):
        root = root_of(s)
        top = max(root, nz - 1 - root)
        held = s % acc.shape[0]
        if k < top:

            @pl.when(((z < root) & (z == k)) | ((z > root) & (nz - 1 - z == k)))
            def _():
                total = acc[held]
                if k > 0:
                    side = jnp.where(z < root, 0, 1)
                    from_side(s, side).wait_recv()
                    total = total + z_in[s, side].astype(jnp.float32)
                z_out[s] = total.astype(jnp.bfloat16)
                inward(s, root).start()

        elif k == top:

            @pl.when(z == root)
            def _():
                total = acc[held]
                for side in range(2):
                    if (root > 0, root < nz - 1)[side]:
                        from_side(s, side).wait_recv()
                        total = total + z_in[s, side].astype(jnp.float32)
                keep = mask[:, (s // 2) * sub:(s // 2 + 1) * sub].astype(jnp.float32)
                out_ref[:, cols(core, s)] = (total * keep * 1.25).astype(jnp.bfloat16)
                if root > 0:
                    outward(s, 0).start()
                if root < nz - 1:
                    outward(s, 1).start()
                to_partner(s).start()

        else:
            away = k - top

            @pl.when((z == root - away) | (z == root + away))
            def _():
                outward(s, 0).wait_recv()

                @pl.when((z < root) & (z > 0))
                def _():
                    outward(s, 0).start()

                @pl.when((z > root) & (z < nz - 1))
                def _():
                    outward(s, 1).start()

                to_partner(s).start()

    def advance(i):
        for k in range(2 * depth, 0, -1):
            s = i - ep_lag - k * z_lag
            if 0 <= s < steps and k <= 2 * max(root_of(s), nz - 1 - root_of(s)):
                chain(s, k)
        s = i - ep_lag
        if 0 <= s < steps:
            combine(s)
            chain(s, 0)

    for s in range(steps):
        pair_out[s] = jnp.dot(hidden[...], w_down[:, cols(1 - core, s)],
                              preferred_element_type=jnp.float32).astype(jnp.bfloat16)
        copy = remote(pair_out.at[s], pair_in.at[s], pair_s.at[0], pair_r.at[s], partner)
        copy.start()
        pair.append(copy)
        if s > 0:
            pair_sum(s - 1)
        mine[s % 2] = jnp.dot(hidden[...], w_down[:, cols(core, s)],
                              preferred_element_type=jnp.float32).astype(jnp.bfloat16)
        advance(s)
    pair_sum(steps - 1)

    for i in range(steps, steps + ep_lag + 2 * depth * z_lag + 1):
        advance(i)
    mine_half = out_ref.at[:, pl.ds(0, half)]
    handed = remote(mine_half, mine_half, gfw_s.at[0], gfw_r.at[0], partner)
    with jax.named_scope("partner_recv"):
        handed.wait_recv()
    with jax.named_scope("sends"):
        handed.wait_send()
        remote(ep_out, ep_out, ep_s.at[0], ep_r.at[0], partner).wait_send()
        remote(pair_out, pair_out, pair_s.at[0], pair_r.at[0], partner).wait_send()
        shared = rows.at[pl.ds(1, n_ep - 1), :, pl.ds(0, groups * sub)]
        remote(shared, shared, share_s.at[0], share_r.at[0], partner).wait_send()
        passed = rows.at[pl.ds(1, n_ep - 1), :, pl.ds(0, half)]
        remote(passed, passed, fwd_s.at[0], fwd_r.at[0], partner).wait_send()
        quarter = out_ref.at[:, pl.ds(0, half // 2)]
        for parity in range(2):
            root = root_of(parity)

            @pl.when(z != root)
            def _():
                sums = z_out.at[pl.ds(0, steps // 2)]
                remote(sums, sums, z_s.at[parity], z_r.at[0, 0], partner).wait_send()

            @pl.when((z <= root) & (z > 0))
            def _():
                remote(quarter, quarter, b_s.at[parity, 0], b_r.at[0], partner).wait_send()

            @pl.when((z >= root) & (z < nz - 1))
            def _():
                remote(quarter, quarter, b_s.at[parity, 1], b_r.at[0], partner).wait_send()


def shards(n_ep, n_tp, tokens, expert_ids, router, gate_weight, up_weight, down_weight, keep_mask):
    experts = router.shape[1]
    toks, width = tokens.shape
    cap = 3 * toks // experts
    nz = n_tp // 2
    total = experts * cap
    sub = 256
    steps = width // 2 // sub
    groups = steps // 3
    w_gate, w_up, w_down = gate_weight[0], up_weight[0], down_weight[0]
    ff = w_gate.shape[1]
    vmem, hbm = pl.BlockSpec(memory_space=pltpu.VMEM), pl.BlockSpec(memory_space=pl.ANY)
    bf = jnp.bfloat16
    dma = pltpu.SemaphoreType.DMA
    return pl.pallas_call(
        functools.partial(kernel, n_ep, nz),
        out_shape=jax.ShapeDtypeStruct((toks, width), bf),
        in_specs=[vmem, vmem, hbm, hbm, hbm, hbm, hbm],
        out_specs=vmem,
        scratch_shapes=[
            pltpu.VMEM((toks, width), bf),
            pltpu.VMEM((width, ff), bf), pltpu.VMEM((width, ff), bf), pltpu.VMEM((ff, width), bf),
            pltpu.VMEM((toks, width // 4), jnp.int32),
            pltpu.VMEM((experts, cap, width), bf),
            pltpu.VMEM((2, total, ff), jnp.float32),
            pltpu.VMEM((total, ff), bf),
            pltpu.VMEM((toks, total), bf),
            pltpu.VMEM((steps, total, sub), bf), pltpu.VMEM((steps, total, sub), bf),
            pltpu.VMEM((2, total, sub), bf),
            pltpu.VMEM((steps, total - cap, sub), bf), pltpu.VMEM((steps, total, sub), bf),
            pltpu.VMEM((steps, toks, sub), bf), pltpu.VMEM((steps, 2, toks, sub), bf),
            pltpu.VMEM((8, toks, sub), jnp.float32),
            dma((3,)), dma((groups,)),
            dma((1,)), dma((2, groups)), dma((1,)), dma((groups,)), dma((1,)), dma((groups,)),
            dma((1,)), dma((steps,)), dma((1,)), dma((steps,)),
            dma((2,)), dma((steps, 2)), dma((2, 2)), dma((steps,)),
            dma((1,)), dma((1,)),
        ],
        compiler_params=pltpu.CompilerParams(
            collective_id=0, has_side_effects=True, vmem_limit_bytes=67043328),
    )(expert_ids.T, router.T, tokens, w_gate, w_up, w_down, keep_mask)


def solution(mesh):
    return jax.shard_map(
        functools.partial(shards, mesh.shape["ep"], mesh.shape["tp"]),
        mesh=mesh,
        in_specs=(
            P("ep", None),
            P("ep", None),
            P(),
            P("ep", None, "tp"),
            P("ep", None, "tp"),
            P("ep", "tp", None),
            P("ep", None),
        ),
        out_specs=P("ep", None),
        check_vma=False,
    )
```

```python
import functools

import jax
import jax.numpy as jnp
from jax import lax
from jax.experimental import pallas as pl
from jax.experimental.pallas import tpu as pltpu
from jax.sharding import PartitionSpec as P

MESH = pl.DeviceIdType.MESH


def flip(index, offset, count):
    out, bit = 0, 1
    while bit < count:
        out = out + ((index // bit + offset // bit) % 2) * bit
        bit *= 2
    return out


def chunk_widths(half, sub):
    return [sub] * (half // sub - 2) + [sub // 2] * 4


def kernel(
    n_ep, nz, ids_ref, router_ref, tokens_hbm, gate_hbm, up_hbm, down_hbm, mask_hbm, out_ref,
    tokens, w_gate, w_up, w_down, mask, rows, gate_up, hidden, comb, pair_out, pair_in, mine, ep_out, ep_in,
    z_out, z_in, far_in, acc, local_sem, w_sem, disp_s, disp_r, share_s, share_r, fwd_s, fwd_r,
    pair_s, pair_r, ep_s, ep_r, z_s, z_r, far_s, far_r, b_s, b_r, gfw_s, gfw_r,
):
    ep, tp = lax.axis_index("ep"), lax.axis_index("tp")
    z, core = tp // 2, tp % 2
    partner = (ep, z * 2 + (1 - core))
    cap, width = rows.shape[1], rows.shape[2]
    toks = out_ref.shape[0]
    ff = w_gate.shape[1]
    half = width // 2
    sub = pair_in.shape[2]
    widths = chunk_widths(half, sub)
    steps, places_of = len(widths), [sum(widths[:n]) for n in range(len(widths))]
    direct = steps - far_in.shape[0]
    groups = fwd_r.shape[1]
    experts = router_ref.shape[0]
    wide = half // groups
    total_rows = n_ep * cap

    def piece(owner_core, s):
        return pl.ds(pl.multiple_of(owner_core * half + s * sub, 128), sub)

    def cols(owner_core, s):
        return pl.ds(pl.multiple_of(owner_core * half + places_of[s], 128), widths[s])

    def own_place(s):
        start = sum(widths[s % 2:s:2])
        return slice(start, start + widths[s])

    def root_of(s):
        return nz // 2 - 1 + (s + core) % 2

    load_tokens = pltpu.make_async_copy(tokens_hbm, tokens, local_sem.at[0])
    load_tokens.start()

    def load_weights(g):
        for h in range(2):
            at = pl.ds(h * half + g * wide, wide)
            for src, dst in ((gate_hbm, w_gate), (up_hbm, w_up)):
                pltpu.make_async_copy(src.at[at], dst.at[at], w_sem.at[g]).start()

    def wait_weights(g):
        at = pl.ds(0, 4 * wide)
        pltpu.make_async_copy(gate_hbm.at[at], w_gate.at[at], w_sem.at[g]).wait()

    load_down = pltpu.make_async_copy(down_hbm, w_down, local_sem.at[1])
    top = nz // 2
    odd_root = (jnp.clip(z - (top - 1), 0, 1) + core) % 2
    load_mask = [pltpu.make_async_copy(mask_hbm.at[:, pl.ds(pl.multiple_of(
        core * half + places_of[2 * j] + odd_root * widths[2 * j], 128), widths[2 * j])],
        mask.at[:, own_place(2 * j)], local_sem.at[2]) for j in range(steps // 2)]

    barrier = pltpu.get_barrier_semaphore()
    peers = [(flip(ep, o, n_ep), tp) for o in range(1, n_ep)] + [partner]
    peers += [(ep, ((z + n) % nz) * 2 + core) for n in range(1, nz)]
    for peer in peers:
        pl.semaphore_signal(barrier, inc=1, device_id=peer, device_id_type=MESH)

    def remote(src, dst, send, recv, device):
        return pltpu.make_async_remote_copy(
            src_ref=src, dst_ref=dst, send_sem=send, recv_sem=recv,
            device_id=device, device_id_type=MESH,
        )

    odd = z % 2
    z_pair = (ep, (z + 1 - 2 * odd) * 2 + core)

    first_id, second_id = ids_ref[0:1, :], ids_ref[1:2, :]
    numbers = lax.broadcasted_iota(jnp.int32, (experts, toks), 0)
    is_first, is_second = numbers == first_id, numbers == second_id
    named = jnp.where(is_first, 1.0, 0.0) + jnp.where(is_second, 1.0, 0.0)
    before = (lax.broadcasted_iota(jnp.int32, (toks, toks), 0) < lax.broadcasted_iota(jnp.int32, (toks, toks), 1))
    ranks = jnp.dot(named.astype(jnp.bfloat16), jnp.where(before, 1.0, 0.0).astype(jnp.bfloat16),
                    preferred_element_type=jnp.float32)

    def of_choice(chosen, values):
        return jnp.sum(jnp.where(chosen, values, 0.0), axis=0, keepdims=True)

    slots = of_choice(is_first, ranks), of_choice(is_second, ranks)
    places = [(number * cap).astype(jnp.float32) + slot for number, slot in zip((first_id, second_id), slots)]

    def picker(owner):
        lines = (lax.broadcasted_iota(jnp.int32, (cap, toks), 0) + owner * cap).astype(jnp.float32)
        return jnp.where((places[0] == lines) | (places[1] == lines), 1.0, 0.0).astype(jnp.bfloat16)

    def piece_of(kind, g):
        return 3 * g + (2 * odd, 1, 2 - 2 * odd)[kind]

    def dispatch(kind, g, o):
        s = piece_of(kind, g)
        return remote(ep_out.at[s, pl.ds((o - 1) * cap, cap), :], rows.at[o, :, piece(core, s)],
                      disp_s.at[0], disp_r.at[kind, g], (flip(ep, o, n_ep), tp))

    def guests(kind, g):
        return rows.at[pl.ds(1, n_ep - 1), :, piece(core, piece_of(kind, g))]

    def share(g):
        return remote(guests(0, g), guests(0, g), share_s.at[0], share_r.at[g], z_pair)

    def forward(kind, g):
        return remote(guests(kind, g), guests(kind, g), fwd_s.at[0], fwd_r.at[kind, g], partner)

    def pass_on(kind, g):
        if kind < 2:
            remote(guests(kind, g), guests(kind, g), disp_s.at[0], disp_r.at[kind, g], partner).wait_recv()
        else:
            share(g).wait_recv()
        if kind == 0:
            share(g).start()
        forward(kind, g).start()

    order = [(0, 0)]
    for g in range(groups):
        if g + 1 < groups:
            order.append((0, g + 1))
        order.append((1, g))
    with jax.named_scope("tokens"):
        load_tokens.wait()
    for g in range(groups):
        load_weights(g)
    others = jnp.concatenate([picker(flip(ep, o, n_ep)) for o in range(1, n_ep)], axis=0)
    for n, (kind, g) in enumerate(order):
        s = piece_of(kind, g)
        ep_out[s] = jnp.dot(others, tokens[:, piece(core, s)],
                            preferred_element_type=jnp.float32).astype(jnp.bfloat16)
        if n == 0:
            with jax.named_scope("barrier"):
                pl.semaphore_wait(barrier, len(peers))
        for o in [n_ep - 1] + list(range(1, n_ep - 1)):
            dispatch(kind, g, o).start()
    load_down.start()
    for load in load_mask:
        load.start()

    own = picker(ep)
    strip = width // 6
    for n in range(6):
        rows[0, :, n * strip:(n + 1) * strip] = jnp.dot(
            own, tokens[:, n * strip:(n + 1) * strip], preferred_element_type=jnp.float32).astype(jnp.bfloat16)

    logits = lax.dot_general(router_ref[...], tokens[...], (((1,), (1,)), ((), ())),
                             preferred_element_type=jnp.float32)
    ahead = of_choice(is_first, logits) - of_choice(is_second, logits)
    lines = lax.broadcasted_iota(jnp.int32, (total_rows, toks), 0).astype(jnp.float32)
    turned = [(jnp.bitwise_xor(number, ep) * cap).astype(jnp.float32) + slot
              for number, slot in zip((first_id, second_id), slots)]
    mixed = (jnp.where(turned[0] == lines, jax.nn.sigmoid(ahead), 0.0)
             + jnp.where(turned[1] == lines, jax.nn.sigmoid(-ahead), 0.0))
    comb[...] = mixed.T.astype(jnp.bfloat16)

    tile = min(256, ff)
    tiles = ff // tile

    def up(pair, lower, upper, first, last):
        for kind, g in pair if lower == 0 else ():
            wait_weights_once(g)
            here = guests(kind, g)
            remote(here, here, fwd_s.at[0], fwd_r.at[kind, g], partner).wait_recv()
        strips = [piece(h, piece_of(kind, g)) for kind, g in pair for h in range(2)]

        def step(n, carry):
            at = pl.ds(pl.multiple_of(n * tile, tile), tile)
            sums = []
            for i, w in enumerate((w_gate, w_up)):
                part = None
                for k in strips:
                    dot = jnp.dot(rows[:, :, k].reshape(total_rows, sub), w[k, at],
                                  preferred_element_type=jnp.float32)
                    part = dot if part is None else part + dot
                if not first:
                    part = part + gate_up[i, :, at]
                if not last:
                    gate_up[i, :, at] = part
                sums.append(part)
            if last:
                hidden[:, at] = (jax.nn.silu(sums[0]) * sums[1]).astype(jnp.bfloat16)
            return carry

        lax.fori_loop(lower, upper, step, 0)

    loaded = set()

    def wait_weights_once(g):
        if g not in loaded:
            loaded.add(g)
            wait_weights(g)

    link, share_link, hop, cross, unit = 2.26, 3.4, 1.8, 1.4, 2.3
    passes, busy = [], 0.0
    for n, (kind, g) in enumerate(order):
        landed = link * (n + 1) + hop
        passes.append((landed, kind, g))
        if kind == 0:
            busy = max(busy, landed) + share_link
            passes.append((busy + hop, 2, g))
    passes.sort()
    due = [(landed, pass_on, (kind, g)) for landed, kind, g in passes]
    clock = 0.0
    for n in range(0, len(passes), 2):
        clock = max(clock, passes[n + 1][0] + cross)
        pair = [given[1:] for given in passes[n:n + 2]]
        for lower, upper in ((0, tiles // 2), (tiles // 2, tiles)):
            due.append((clock, up, (pair, lower, upper, n == 0, n + 2 == len(passes))))
            clock += unit / 2
    for _, action, given in sorted(due, key=lambda event: event[0]):
        with jax.named_scope(action.__name__ + "_".join(str(x) for x in given[:2]).replace(" ", "")):
            action(*given)

    load_down.wait()
    pltpu.make_async_copy(mask_hbm.at[:, 0:mask.shape[1]], mask, local_sem.at[2]).wait()
    staged = ep_out.at[pl.ds(0, len(order))]
    remote(staged, staged, disp_s.at[0], disp_r.at[0, 0], partner).wait_send()

    def within(s):
        return pl.ds(places_of[s] % sub, widths[s])

    def box(s):
        return places_of[s] // sub

    def to_pair(s):
        return remote(pair_out.at[box(s), :, within(s)], pair_in.at[box(s), :, within(s)], pair_s.at[0], pair_r.at[s], partner)

    def down(s):
        pair_out[box(s), :, within(s)] = jnp.dot(hidden[...], w_down[:, cols(1 - core, s)],
                                            preferred_element_type=jnp.float32).astype(jnp.bfloat16)
        mine[s % 2, :, within(s)] = jnp.dot(hidden[...], w_down[:, cols(core, s)],
                                            preferred_element_type=jnp.float32).astype(jnp.bfloat16)
        to_pair(s).start()
        if s > 0:
            pair_sum(s - 1)
        if s == steps - 1:
            pair_sum(s)

    def pair_sum(s):
        at = within(s)
        to_pair(s).wait_recv()
        summed = (mine[s % 2, :, at].astype(jnp.float32) + pair_in[box(s), :, at].astype(jnp.float32)).astype(jnp.bfloat16)
        ep_in[box(s), 0:cap, at] = summed[0:cap]
        ep_out[box(s), :, at] = summed[cap:]
        for o in range(1, n_ep):
            remote(ep_out.at[box(s), pl.ds((o - 1) * cap, cap), at], ep_in.at[box(s), pl.ds(o * cap, cap), at],
                   ep_s.at[0], ep_r.at[s], (flip(ep, o, n_ep), tp)).start()

    def inward(s, root):
        side = jnp.where(z < root, 0, 1)
        to = jnp.where(z < root, z + 1, z - 1)
        return remote(z_out.at[box(s)], z_in.at[s, side], z_s.at[s % 2], z_r.at[s, side], (ep, to * 2 + core))

    def from_side(s, side):
        return remote(z_out.at[box(s)], z_in.at[s, side], z_s.at[s % 2], z_r.at[s, side], partner)

    def outward(s, side):
        here = out_ref.at[:, cols(core, s)]
        return remote(here, here, b_s.at[s % 2, side], b_r.at[s], (ep, (z - 1 + 2 * side) * 2 + core))

    def to_partner(s):
        here = out_ref.at[:, cols(core, s)]
        return remote(here, here, gfw_s.at[0], gfw_r.at[0], partner)

    def finish(s, total):
        keep = mask[:, own_place(s)].astype(jnp.float32)
        out_ref[:, cols(core, s)] = (total * keep * 1.25).astype(jnp.bfloat16)

    def combine(s):
        at = within(s)
        arrived = ep_in.at[box(s), pl.ds(cap, total_rows - cap), at]
        remote(arrived, arrived, ep_s.at[0], ep_r.at[s], partner).wait_recv()
        acc[s % acc.shape[0], :, at] = jnp.dot(comb[...], ep_in[box(s), :, at], preferred_element_type=jnp.float32)

    def straight(s, k):
        root, n, at = root_of(s), s - direct, within(s)
        held = s % acc.shape[0]
        if k == 0:

            @pl.when(z != root)
            def _():
                z_out[box(s), :, at] = acc[held, :, at].astype(jnp.bfloat16)
                slot = jnp.where(z < root, z, z - 1)
                remote(z_out.at[box(s), :, at], far_in.at[n, slot], z_s.at[s % 2], far_r.at[n],
                       (ep, root * 2 + core)).start()

        elif k == 1:

            @pl.when(z == root)
            def _():
                parts = far_in.at[n]
                remote(parts, parts, z_s.at[0], far_r.at[n], partner).wait_recv()
                total = acc[held, :, at]
                for slot in range(nz - 1):
                    total = total + far_in[n, slot].astype(jnp.float32)
                finish(s, total)
                here = out_ref.at[:, cols(core, s)]
                for other in range(1, nz):
                    remote(here, here, far_s.at[s % 2], b_r.at[s], (ep, ((root + other) % nz) * 2 + core)).start()
                to_partner(s).start()

        else:

            @pl.when(z != root)
            def _():
                outward(s, 0).wait_recv()
                to_partner(s).start()

    def chain(s, k, at_end=False):
        root = root_of(s)
        held = s % acc.shape[0]
        if k < top:

            @pl.when(((z < root) & (z == k)) | ((z > root) & (nz - 1 - z == k)))
            def _():
                total = acc[held]
                if k > 0:
                    side = jnp.where(z < root, 0, 1)
                    from_side(s, side).wait_recv()
                    total = total + z_in[s, side].astype(jnp.float32)
                z_out[box(s)] = total.astype(jnp.bfloat16)
                inward(s, root).start()

        elif k == top:

            @pl.when(z == root)
            def _():
                total = acc[held]
                for side in range(2):
                    from_side(s, side).wait_recv()
                    total = total + z_in[s, side].astype(jnp.float32)
                finish(s, total)
                outward(s, 0).start()
                outward(s, 1).start()
                to_partner(s).start()

        else:
            away = k - top

            end = (z == 0) | (z == nz - 1)

            @pl.when(((z == root - away) | (z == root + away)) & (end if at_end else jnp.logical_not(end)))
            def _():
                outward(s, 0).wait_recv()

                @pl.when((z < root) & (z > 0))
                def _():
                    outward(s, 0).start()

                @pl.when((z > root) & (z < nz - 1))
                def _():
                    outward(s, 1).start()

                to_partner(s).start()

    due = []
    landed = 4.5
    finish_at = landed + link * half / sub
    for s in range(steps):
        landed += link * widths[s] / sub
        due.append((max(0.01 * s, landed - 14.0), down, (s,)))
        due.append((landed, combine, (s,)))
        if s < direct:
            for k in range(2 * top + 1):
                due.append((landed + 0.1 + 3.6 * k, chain, (s, k)))
                if k > top:
                    late = landed + 0.1 + 3.6 * k + 4
                    due.append((late if late < finish_at - 2 else max(late, finish_at + 0.2), chain, (s, k, True)))
        else:
            for k in range(3):
                due.append((landed + 0.1 + 5.0 * k, straight, (s, k)))
    for _, action, given in sorted(due, key=lambda event: event[0]):
        with jax.named_scope(action.__name__ + "_".join(str(x) for x in given)):
            action(*given)

    mine_half = out_ref.at[:, pl.ds(0, half)]
    handed = remote(mine_half, mine_half, gfw_s.at[0], gfw_r.at[0], partner)
    with jax.named_scope("partner_recv"):
        handed.wait_recv()
    with jax.named_scope("sends"):
        handed.wait_send()
        full = pl.ds(0, half // sub)
        remote(ep_out.at[full], ep_out.at[full], ep_s.at[0], ep_r.at[0], partner).wait_send()
        remote(pair_out.at[full], pair_out.at[full], pair_s.at[0], pair_r.at[0], partner).wait_send()
        shared = rows.at[pl.ds(1, n_ep - 1), :, pl.ds(0, groups * sub)]
        remote(shared, shared, share_s.at[0], share_r.at[0], partner).wait_send()
        passed = rows.at[pl.ds(1, n_ep - 1), :, pl.ds(0, half)]
        remote(passed, passed, fwd_s.at[0], fwd_r.at[0, 0], partner).wait_send()
        chained = out_ref.at[:, pl.ds(0, sum(widths[:direct]) // 2)]
        spread = out_ref.at[:, pl.ds(0, sum(widths[direct:]) // 2 * (nz - 1))]
        for parity in range(2):
            root = root_of(parity)

            @pl.when(z != root)
            def _():
                sums = z_out.at[pl.ds(0, half // sub // 2)]
                remote(sums, sums, z_s.at[parity], z_r.at[0, 0], partner).wait_send()

            @pl.when(z == root)
            def _():
                remote(spread, spread, far_s.at[parity], b_r.at[0], partner).wait_send()

            @pl.when((z <= root) & (z > 0))
            def _():
                remote(chained, chained, b_s.at[parity, 0], b_r.at[0], partner).wait_send()

            @pl.when((z >= root) & (z < nz - 1))
            def _():
                remote(chained, chained, b_s.at[parity, 1], b_r.at[0], partner).wait_send()


def shards(n_ep, n_tp, tokens, expert_ids, router, gate_weight, up_weight, down_weight, keep_mask):
    experts = router.shape[1]
    toks, width = tokens.shape
    cap = 3 * toks // experts
    nz = n_tp // 2
    total = experts * cap
    sub = 256
    groups = width // 2 // sub // 3
    boxes = width // 2 // sub
    steps, far = len(chunk_widths(width // 2, sub)), 4
    w_gate, w_up, w_down = gate_weight[0], up_weight[0], down_weight[0]
    ff = w_gate.shape[1]
    vmem, hbm = pl.BlockSpec(memory_space=pltpu.VMEM), pl.BlockSpec(memory_space=pl.ANY)
    bf = jnp.bfloat16
    dma = pltpu.SemaphoreType.DMA
    return pl.pallas_call(
        functools.partial(kernel, n_ep, nz),
        out_shape=pltpu.VMEM((toks, width), bf),
        in_specs=[vmem, vmem, hbm, hbm, hbm, hbm, hbm],
        out_specs=vmem,
        scratch_shapes=[
            pltpu.VMEM((toks, width), bf),
            pltpu.VMEM((width, ff), bf), pltpu.VMEM((width, ff), bf), pltpu.VMEM((ff, width), bf),
            pltpu.VMEM((toks, width // 4), jnp.int32),
            pltpu.VMEM((experts, cap, width), bf),
            pltpu.VMEM((2, total, ff), jnp.float32),
            pltpu.VMEM((total, ff), bf),
            pltpu.VMEM((toks, total), bf),
            pltpu.VMEM((boxes, total, sub), bf), pltpu.VMEM((boxes, total, sub), bf),
            pltpu.VMEM((2, total, sub), bf),
            pltpu.VMEM((boxes, total - cap, sub), bf), pltpu.VMEM((boxes, total, sub), bf),
            pltpu.VMEM((boxes, toks, sub), bf), pltpu.VMEM((steps - far, 2, toks, sub), bf),
            pltpu.VMEM((far, nz - 1, toks, sub // 2), bf),
            pltpu.VMEM((8 if nz <= 4 else 10, toks, sub), jnp.float32),
            dma((3,)), dma((groups,)),
            dma((1,)), dma((2, groups)), dma((1,)), dma((groups,)), dma((1,)), dma((3, groups)),
            dma((1,)), dma((steps,)), dma((1,)), dma((steps,)),
            dma((2,)), dma((steps - far, 2)), dma((2,)), dma((far,)), dma((2, 2)), dma((steps,)),
            dma((1,)), dma((1,)),
        ],
        compiler_params=pltpu.CompilerParams(
            collective_id=0, has_side_effects=True, vmem_limit_bytes=65200000),
    )(expert_ids.T, router.T, tokens, w_gate, w_up, w_down, keep_mask)


def solution(mesh):
    return jax.shard_map(
        functools.partial(shards, mesh.shape["ep"], mesh.shape["tp"]),
        mesh=mesh,
        in_specs=(
            P("ep", None),
            P("ep", None),
            P(),
            P("ep", None, "tp"),
            P("ep", None, "tp"),
            P("ep", "tp", None),
            P("ep", None),
        ),
        out_specs=P("ep", None),
        check_vma=False,
    )
```

```python
import functools

import jax
import jax.numpy as jnp
from jax import lax
from jax.experimental import pallas as pl
from jax.experimental.pallas import tpu as pltpu
from jax.sharding import PartitionSpec as P

MESH = pl.DeviceIdType.MESH


def flip(index, offset, count):
    out, bit = 0, 1
    while bit < count:
        out = out + ((index // bit + offset // bit) % 2) * bit
        bit *= 2
    return out


def chunk_widths(half, sub):
    return [sub] * (half // sub - 4) + [sub // 2] * 8


def kernel(
    n_ep, nz, ids_ref, router_ref, tokens_hbm, gate_hbm, up_hbm, down_hbm, mask_hbm, out_ref,
    tokens, w_gate, w_up, w_down, mask, rows, gate_up, hidden, comb, pair_out, pair_in, mine, ep_out, ep_in,
    z_out, z_in, far_in, acc, local_sem, w_sem, disp_s, disp_r, share_s, share_r, fwd_s, fwd_r,
    pair_s, pair_r, ep_s, ep_r, z_s, z_r, far_s, far_r, b_s, b_r, gfw_s, gfw_r,
):
    ep, tp = lax.axis_index("ep"), lax.axis_index("tp")
    z, core = tp // 2, tp % 2
    partner = (ep, z * 2 + (1 - core))
    cap, width = rows.shape[1], rows.shape[2]
    toks = out_ref.shape[0]
    ff = w_gate.shape[1]
    half = width // 2
    sub = pair_in.shape[2]
    widths = chunk_widths(half, sub)
    steps, places_of = len(widths), [sum(widths[:n]) for n in range(len(widths))]
    direct = steps - far_in.shape[0]
    groups = fwd_r.shape[1]
    experts = router_ref.shape[0]
    wide = half // groups
    total_rows = n_ep * cap

    def piece(owner_core, s):
        return pl.ds(pl.multiple_of(owner_core * half + s * sub, 128), sub)

    def cols(owner_core, s):
        return pl.ds(pl.multiple_of(owner_core * half + places_of[s], 128), widths[s])

    def own_place(s):
        start = sum(widths[s % 2:s:2])
        return slice(start, start + widths[s])

    def root_of(s):
        return nz // 2 - 1 + (s + core) % 2

    load_tokens = pltpu.make_async_copy(tokens_hbm, tokens, local_sem.at[0])
    load_tokens.start()

    def load_weights(g):
        for h in range(2):
            at = pl.ds(h * half + g * wide, wide)
            for src, dst in ((gate_hbm, w_gate), (up_hbm, w_up)):
                pltpu.make_async_copy(src.at[at], dst.at[at], w_sem.at[g]).start()

    def wait_weights(g):
        at = pl.ds(0, 4 * wide)
        pltpu.make_async_copy(gate_hbm.at[at], w_gate.at[at], w_sem.at[g]).wait()

    load_down = pltpu.make_async_copy(down_hbm, w_down, local_sem.at[1])
    top = nz // 2
    odd_root = (jnp.clip(z - (top - 1), 0, 1) + core) % 2
    load_mask = [pltpu.make_async_copy(mask_hbm.at[:, pl.ds(pl.multiple_of(
        core * half + places_of[2 * j] + odd_root * widths[2 * j], 128), widths[2 * j])],
        mask.at[:, own_place(2 * j)], local_sem.at[2]) for j in range(steps // 2)]

    barrier = pltpu.get_barrier_semaphore()
    peers = [(flip(ep, o, n_ep), tp) for o in range(1, n_ep)] + [partner]
    peers += [(ep, ((z + n) % nz) * 2 + core) for n in range(1, nz)]
    for peer in peers:
        pl.semaphore_signal(barrier, inc=1, device_id=peer, device_id_type=MESH)

    def remote(src, dst, send, recv, device):
        return pltpu.make_async_remote_copy(
            src_ref=src, dst_ref=dst, send_sem=send, recv_sem=recv,
            device_id=device, device_id_type=MESH,
        )

    odd = z % 2
    z_pair = (ep, (z + 1 - 2 * odd) * 2 + core)

    first_id, second_id = ids_ref[0:1, :], ids_ref[1:2, :]
    numbers = lax.broadcasted_iota(jnp.int32, (experts, toks), 0)
    is_first, is_second = numbers == first_id, numbers == second_id
    named = jnp.where(is_first, 1.0, 0.0) + jnp.where(is_second, 1.0, 0.0)
    before = (lax.broadcasted_iota(jnp.int32, (toks, toks), 0) < lax.broadcasted_iota(jnp.int32, (toks, toks), 1))
    ranks = jnp.dot(named.astype(jnp.bfloat16), jnp.where(before, 1.0, 0.0).astype(jnp.bfloat16),
                    preferred_element_type=jnp.float32)

    def of_choice(chosen, values):
        return jnp.sum(jnp.where(chosen, values, 0.0), axis=0, keepdims=True)

    slots = of_choice(is_first, ranks), of_choice(is_second, ranks)
    places = [(number * cap).astype(jnp.float32) + slot for number, slot in zip((first_id, second_id), slots)]

    def picker(owner):
        lines = (lax.broadcasted_iota(jnp.int32, (cap, toks), 0) + owner * cap).astype(jnp.float32)
        return jnp.where((places[0] == lines) | (places[1] == lines), 1.0, 0.0).astype(jnp.bfloat16)

    def piece_of(kind, g):
        return 3 * g + (2 * odd, 1, 2 - 2 * odd)[kind]

    def dispatch(kind, g, o):
        s = piece_of(kind, g)
        return remote(ep_out.at[s, pl.ds((o - 1) * cap, cap), :], rows.at[o, :, piece(core, s)],
                      disp_s.at[0], disp_r.at[kind, g], (flip(ep, o, n_ep), tp))

    def guests(kind, g):
        return rows.at[pl.ds(1, n_ep - 1), :, piece(core, piece_of(kind, g))]

    def share(g):
        return remote(guests(0, g), guests(0, g), share_s.at[0], share_r.at[g], z_pair)

    def forward(kind, g):
        return remote(guests(kind, g), guests(kind, g), fwd_s.at[0], fwd_r.at[kind, g], partner)

    def pass_on(kind, g):
        if kind < 2:
            remote(guests(kind, g), guests(kind, g), disp_s.at[0], disp_r.at[kind, g], partner).wait_recv()
        else:
            share(g).wait_recv()
        if kind == 0:
            share(g).start()
        forward(kind, g).start()

    order = [(0, g) for g in range(2)]
    for g in range(groups):
        if g + 2 < groups:
            order.append((0, g + 2))
        order.append((1, g))
    with jax.named_scope("tokens"):
        load_tokens.wait()
    for g in range(groups):
        load_weights(g)
    others = jnp.concatenate([picker(flip(ep, o, n_ep)) for o in range(1, n_ep)], axis=0)
    for n, (kind, g) in enumerate(order):
        s = piece_of(kind, g)
        ep_out[s] = jnp.dot(others, tokens[:, piece(core, s)],
                            preferred_element_type=jnp.float32).astype(jnp.bfloat16)
        if n == 0:
            with jax.named_scope("barrier"):
                pl.semaphore_wait(barrier, len(peers))
        for o in [n_ep - 1] + list(range(1, n_ep - 1)):
            dispatch(kind, g, o).start()
    load_down.start()
    for load in load_mask:
        load.start()

    own = picker(ep)
    strip = width // 6
    for n in range(6):
        rows[0, :, n * strip:(n + 1) * strip] = jnp.dot(
            own, tokens[:, n * strip:(n + 1) * strip], preferred_element_type=jnp.float32).astype(jnp.bfloat16)

    logits = lax.dot_general(router_ref[...], tokens[...], (((1,), (1,)), ((), ())),
                             preferred_element_type=jnp.float32)
    ahead = of_choice(is_first, logits) - of_choice(is_second, logits)
    lines = lax.broadcasted_iota(jnp.int32, (total_rows, toks), 0).astype(jnp.float32)
    turned = [(jnp.bitwise_xor(number, ep) * cap).astype(jnp.float32) + slot
              for number, slot in zip((first_id, second_id), slots)]
    mixed = (jnp.where(turned[0] == lines, jax.nn.sigmoid(ahead), 0.0)
             + jnp.where(turned[1] == lines, jax.nn.sigmoid(-ahead), 0.0))
    comb[...] = mixed.T.astype(jnp.bfloat16)

    tile = min(256, ff)
    tiles = ff // tile

    def up(pair, lower, upper, first, last):
        for kind, g in pair if lower == 0 else ():
            wait_weights_once(g)
            here = guests(kind, g)
            remote(here, here, fwd_s.at[0], fwd_r.at[kind, g], partner).wait_recv()
        strips = [piece(h, piece_of(kind, g)) for kind, g in pair for h in range(2)]

        def step(n, carry):
            at = pl.ds(pl.multiple_of(n * tile, tile), tile)
            sums = []
            for i, w in enumerate((w_gate, w_up)):
                part = None
                for k in strips:
                    dot = jnp.dot(rows[:, :, k].reshape(total_rows, sub), w[k, at],
                                  preferred_element_type=jnp.float32)
                    part = dot if part is None else part + dot
                if not first:
                    part = part + gate_up[i, :, at]
                if not last:
                    gate_up[i, :, at] = part
                sums.append(part)
            if last:
                hidden[:, at] = (jax.nn.silu(sums[0]) * sums[1]).astype(jnp.bfloat16)
            return carry

        lax.fori_loop(lower, upper, step, 0)

    loaded = set()

    def wait_weights_once(g):
        if g not in loaded:
            loaded.add(g)
            wait_weights(g)

    link, share_link, hop, cross, unit = 2.26, 3.4, 3.0, 1.4, 2.3
    passes, busy = [], 0.0
    for n, (kind, g) in enumerate(order):
        landed = link * (n + 1) + hop
        passes.append((landed, kind, g))
        if kind == 0:
            busy = max(busy, landed) + share_link
            passes.append((busy + hop, 2, g))
    passes.sort()
    due = [(landed, pass_on, (kind, g)) for landed, kind, g in passes]
    clock = 0.0
    for n in range(0, len(passes), 2):
        clock = max(clock, passes[n + 1][0] + cross)
        pair = [given[1:] for given in passes[n:n + 2]]
        for lower, upper in ((0, tiles // 2), (tiles // 2, tiles)):
            due.append((clock, up, (pair, lower, upper, n == 0, n + 2 == len(passes))))
            clock += unit / 2
    for _, action, given in sorted(due, key=lambda event: event[0]):
        with jax.named_scope(action.__name__ + "_".join(str(x) for x in given[:2]).replace(" ", "")):
            action(*given)

    load_down.wait()
    pltpu.make_async_copy(mask_hbm.at[:, 0:mask.shape[1]], mask, local_sem.at[2]).wait()
    staged = ep_out.at[pl.ds(0, len(order))]
    remote(staged, staged, disp_s.at[0], disp_r.at[0, 0], partner).wait_send()

    def within(s):
        return pl.ds(places_of[s] % sub, widths[s])

    def box(s):
        return places_of[s] // sub

    def to_pair(s):
        return remote(pair_out.at[box(s), :, within(s)], pair_in.at[box(s), :, within(s)], pair_s.at[0], pair_r.at[s], partner)

    def down(s):
        pair_out[box(s), :, within(s)] = jnp.dot(hidden[...], w_down[:, cols(1 - core, s)],
                                            preferred_element_type=jnp.float32).astype(jnp.bfloat16)
        mine[s % 2, :, within(s)] = jnp.dot(hidden[...], w_down[:, cols(core, s)],
                                            preferred_element_type=jnp.float32).astype(jnp.bfloat16)
        to_pair(s).start()
        if s > 0:
            pair_sum(s - 1)
        if s == steps - 1:
            pair_sum(s)

    def pair_sum(s):
        at = within(s)
        to_pair(s).wait_recv()
        summed = (mine[s % 2, :, at].astype(jnp.float32) + pair_in[box(s), :, at].astype(jnp.float32)).astype(jnp.bfloat16)
        ep_in[box(s), 0:cap, at] = summed[0:cap]
        ep_out[box(s), :, at] = summed[cap:]
        for o in range(1, n_ep):
            remote(ep_out.at[box(s), pl.ds((o - 1) * cap, cap), at], ep_in.at[box(s), pl.ds(o * cap, cap), at],
                   ep_s.at[0], ep_r.at[s], (flip(ep, o, n_ep), tp)).start()

    def inward(s, root):
        side = jnp.where(z < root, 0, 1)
        to = jnp.where(z < root, z + 1, z - 1)
        at = within(s)
        return remote(z_out.at[box(s), :, at], z_in.at[s, side, :, at], z_s.at[s % 2], z_r.at[s, side],
                      (ep, to * 2 + core))

    def from_side(s, side):
        at = within(s)
        return remote(z_out.at[box(s), :, at], z_in.at[s, side, :, at], z_s.at[s % 2], z_r.at[s, side], partner)

    def outward(s, side):
        here = out_ref.at[:, cols(core, s)]
        return remote(here, here, b_s.at[s % 2, side], b_r.at[s], (ep, (z - 1 + 2 * side) * 2 + core))

    def to_partner(s):
        here = out_ref.at[:, cols(core, s)]
        return remote(here, here, gfw_s.at[0], gfw_r.at[0], partner)

    def finish(s, total):
        keep = mask[:, own_place(s)].astype(jnp.float32)
        out_ref[:, cols(core, s)] = (total * keep * 1.25).astype(jnp.bfloat16)

    def combine(s):
        at = within(s)
        arrived = ep_in.at[box(s), pl.ds(cap, total_rows - cap), at]
        remote(arrived, arrived, ep_s.at[0], ep_r.at[s], partner).wait_recv()
        acc[s % acc.shape[0], :, at] = jnp.dot(comb[...], ep_in[box(s), :, at], preferred_element_type=jnp.float32)

    def straight(s, k):
        root, n, at = root_of(s), s - direct, within(s)
        held = s % acc.shape[0]
        if k == 0:

            @pl.when(z != root)
            def _():
                z_out[box(s), :, at] = acc[held, :, at].astype(jnp.bfloat16)
                slot = jnp.where(z < root, z, z - 1)
                remote(z_out.at[box(s), :, at], far_in.at[n, slot], z_s.at[s % 2], far_r.at[n],
                       (ep, root * 2 + core)).start()

        elif k == 1:

            @pl.when(z == root)
            def _():
                parts = far_in.at[n]
                remote(parts, parts, z_s.at[0], far_r.at[n], partner).wait_recv()
                total = acc[held, :, at]
                for slot in range(nz - 1):
                    total = total + far_in[n, slot].astype(jnp.float32)
                finish(s, total)
                here = out_ref.at[:, cols(core, s)]
                for other in range(1, nz):
                    remote(here, here, far_s.at[s % 2], b_r.at[s], (ep, ((root + other) % nz) * 2 + core)).start()
                to_partner(s).start()

        else:

            @pl.when(z != root)
            def _():
                outward(s, 0).wait_recv()
                to_partner(s).start()

    def chain(s, k, at_end=False):
        root = root_of(s)
        held, at = s % acc.shape[0], within(s)
        if k < top:

            @pl.when(((z < root) & (z == k)) | ((z > root) & (nz - 1 - z == k)))
            def _():
                total = acc[held, :, at]
                if k > 0:
                    side = jnp.where(z < root, 0, 1)
                    from_side(s, side).wait_recv()
                    total = total + z_in[s, side, :, at].astype(jnp.float32)
                z_out[box(s), :, at] = total.astype(jnp.bfloat16)
                inward(s, root).start()

        elif k == top:

            @pl.when(z == root)
            def _():
                total = acc[held, :, at]
                for side in range(2):
                    from_side(s, side).wait_recv()
                    total = total + z_in[s, side, :, at].astype(jnp.float32)
                finish(s, total)
                outward(s, 0).start()
                outward(s, 1).start()
                to_partner(s).start()

        else:
            away = k - top

            end = (z == 0) | (z == nz - 1)

            @pl.when(((z == root - away) | (z == root + away)) & (end if at_end else jnp.logical_not(end)))
            def _():
                outward(s, 0).wait_recv()

                @pl.when((z < root) & (z > 0))
                def _():
                    outward(s, 0).start()

                @pl.when((z > root) & (z < nz - 1))
                def _():
                    outward(s, 1).start()

                to_partner(s).start()

    due = []
    landed = 4.5
    finish_at = landed + link * half / sub
    for s in range(steps):
        landed += link * widths[s] / sub
        due.append((max(0.01 * s, landed - 14.0), down, (s,)))
        due.append((landed, combine, (s,)))
        if s < direct:
            for k in range(2 * top + 1):
                due.append((landed + 0.1 + 3.6 * k, chain, (s, k)))
                if k > top:
                    late = landed + 0.1 + 3.6 * k + 4
                    due.append((late if late < finish_at - 2 else max(late, finish_at + 0.2), chain, (s, k, True)))
        else:
            for k in range(3):
                due.append((landed + 0.1 + 5.0 * k, straight, (s, k)))
    for _, action, given in sorted(due, key=lambda event: event[0]):
        with jax.named_scope(action.__name__ + "_".join(str(x) for x in given)):
            action(*given)

    mine_half = out_ref.at[:, pl.ds(0, half)]
    handed = remote(mine_half, mine_half, gfw_s.at[0], gfw_r.at[0], partner)
    with jax.named_scope("partner_recv"):
        handed.wait_recv()
    with jax.named_scope("sends"):
        handed.wait_send()
        full = pl.ds(0, half // sub)
        remote(ep_out.at[full], ep_out.at[full], ep_s.at[0], ep_r.at[0], partner).wait_send()
        remote(pair_out.at[full], pair_out.at[full], pair_s.at[0], pair_r.at[0], partner).wait_send()
        shared = rows.at[pl.ds(1, n_ep - 1), :, pl.ds(0, groups * sub)]
        remote(shared, shared, share_s.at[0], share_r.at[0], partner).wait_send()
        passed = rows.at[pl.ds(1, n_ep - 1), :, pl.ds(0, half)]
        remote(passed, passed, fwd_s.at[0], fwd_r.at[0, 0], partner).wait_send()
        chained = out_ref.at[:, pl.ds(0, sum(widths[:direct]) // 2)]
        spread = out_ref.at[:, pl.ds(0, sum(widths[direct:]) // 2 * (nz - 1))]
        for parity in range(2):
            root = root_of(parity)

            @pl.when(z != root)
            def _():
                sums = z_out.at[pl.ds(0, half // sub // 2)]
                remote(sums, sums, z_s.at[parity], z_r.at[0, 0], partner).wait_send()

            @pl.when(z == root)
            def _():
                remote(spread, spread, far_s.at[parity], b_r.at[0], partner).wait_send()

            @pl.when((z <= root) & (z > 0))
            def _():
                remote(chained, chained, b_s.at[parity, 0], b_r.at[0], partner).wait_send()

            @pl.when((z >= root) & (z < nz - 1))
            def _():
                remote(chained, chained, b_s.at[parity, 1], b_r.at[0], partner).wait_send()


def shards(n_ep, n_tp, tokens, expert_ids, router, gate_weight, up_weight, down_weight, keep_mask):
    experts = router.shape[1]
    toks, width = tokens.shape
    cap = 3 * toks // experts
    nz = n_tp // 2
    total = experts * cap
    sub = 256
    groups = width // 2 // sub // 3
    boxes = width // 2 // sub
    steps, far = len(chunk_widths(width // 2, sub)), 4
    w_gate, w_up, w_down = gate_weight[0], up_weight[0], down_weight[0]
    ff = w_gate.shape[1]
    vmem, hbm = pl.BlockSpec(memory_space=pltpu.VMEM), pl.BlockSpec(memory_space=pl.ANY)
    bf = jnp.bfloat16
    dma = pltpu.SemaphoreType.DMA
    return pl.pallas_call(
        functools.partial(kernel, n_ep, nz),
        out_shape=pltpu.VMEM((toks, width), bf),
        in_specs=[vmem, vmem, hbm, hbm, hbm, hbm, hbm],
        out_specs=vmem,
        scratch_shapes=[
            pltpu.VMEM((toks, width), bf),
            pltpu.VMEM((width, ff), bf), pltpu.VMEM((width, ff), bf), pltpu.VMEM((ff, width), bf),
            pltpu.VMEM((toks, width // 4), jnp.int32),
            pltpu.VMEM((experts, cap, width), bf),
            pltpu.VMEM((2, total, ff), jnp.float32),
            pltpu.VMEM((total, ff), bf),
            pltpu.VMEM((toks, total), bf),
            pltpu.VMEM((boxes, total, sub), bf), pltpu.VMEM((boxes, total, sub), bf),
            pltpu.VMEM((2, total, sub), bf),
            pltpu.VMEM((boxes, total - cap, sub), bf), pltpu.VMEM((boxes, total, sub), bf),
            pltpu.VMEM((boxes, toks, sub), bf), pltpu.VMEM((steps - far, 2, toks, sub), bf),
            pltpu.VMEM((far, nz - 1, toks, sub // 2), bf),
            pltpu.VMEM((8 if nz <= 4 else 12, toks, sub), jnp.float32),
            dma((3,)), dma((groups,)),
            dma((1,)), dma((2, groups)), dma((1,)), dma((groups,)), dma((1,)), dma((3, groups)),
            dma((1,)), dma((steps,)), dma((1,)), dma((steps,)),
            dma((2,)), dma((steps - far, 2)), dma((2,)), dma((far,)), dma((2, 2)), dma((steps,)),
            dma((1,)), dma((1,)),
        ],
        compiler_params=pltpu.CompilerParams(
            collective_id=0, has_side_effects=True, vmem_limit_bytes=65200000),
    )(expert_ids.T, router.T, tokens, w_gate, w_up, w_down, keep_mask)


def solution(mesh):
    return jax.shard_map(
        functools.partial(shards, mesh.shape["ep"], mesh.shape["tp"]),
        mesh=mesh,
        in_specs=(
            P("ep", None),
            P("ep", None),
            P(),
            P("ep", None, "tp"),
            P("ep", None, "tp"),
            P("ep", "tp", None),
            P("ep", None),
        ),
        out_specs=P("ep", None),
        check_vma=False,
    )
```
